512 devices in a mesh: grp: 16 (over z), dp: 32 (over x, y, core).
Axes of the slice: x: 4, y: 4, z: 16, core: 2. Of those that a mesh axis runs over, the one named last changes fastest.
Arguments:
- tokens: bfloat16 [65536, 3584], P(('grp', 'dp')), may hold values from -120 to 120, as said below
- lengths: int32 [512, 4], P(('grp', 'dp')), may hold values from 0 to 128, as said below
- dest: int32 [512, 4], P(('grp', 'dp')), may hold values from -1 to 15, as said below
- gain: float32 [3584], replicated, may hold values from 0.5 to 1.5
- weight: bfloat16 [3584, 10240], P('dp', 'grp'), may hold values from -0.09375 to 0.09375
Outputs:
- projected: bfloat16 [32768, 10240], P('dp', 'grp')
The draws below stay inside these ranges and needn't reach their ends.
Inputs may be any that keep to these rules, and one draw needn't show every extreme that they name: The tokens of one row have a common scale, and so have those of one feature. A device's live rows are the sum of its lengths; rows after them are padding. Within the devices sharing a dp index, live rows fill ceil(live rows / 32) blocks on each device and 32 blocks in all. dest is -1 exactly for a device's blocks past its live rows and an owner along grp otherwise. Within the devices sharing a dp index, every owner receives exactly 2 blocks and no device sends more than 1 block to one owner.
All inputs are finite; a program needn't handle non-finite values.
Results may differ from the reference program's by a relative error of at most 0.0049.
Values may be sent and summed in bfloat16 or wider, within the bound.
No kernel may reach another device: no remote copies, remote signals or barrier semaphores. Data moves between devices by JAX's collectives and lax.ppermute only.
A program may use at most 64 MiB of HBM per device.

```python
import math
import jax
import jax.numpy as jnp
from jax import lax

D = 3584
FF = 10240
BLK = 32
DOCS = 4
OWN_BLK = 2
IN_BLK = 4
ROWS_GRP = 1024
TOKENS = 65536
N_GRP = 16
N_DP = 32


def shared_layout(key):
    base = jax.random.fold_in(key, 7001)
    slots_in = 2 * OWN_BLK

    def one_group(group_key):
        keys = jax.random.split(group_key, 5)
        order = jax.random.permutation(keys[0], N_GRP)
        steps = jax.random.randint(keys[1], (N_GRP // 2,), 0, OWN_BLK + 1)
        steps = steps.at[0].set(OWN_BLK)
        delta = jnp.zeros((N_GRP,), jnp.int32)
        delta = delta.at[order[0::2]].set(steps).at[order[1::2]].set(-steps)
        counts = OWN_BLK + delta
        extra = jax.random.randint(keys[2], (N_GRP,), 1, BLK + 1)
        extra = extra.at[order[0]].set(BLK)
        live_rows = jnp.where(counts > 0, (counts - 1) * BLK + extra, 0)
        cuts = jax.random.randint(keys[3], (N_GRP, DOCS - 1), 0, live_rows[:, None] + 1)
        cuts = jnp.sort(cuts, axis=1)
        cuts = cuts.at[order[0]].set(0)
        bounds = jnp.concatenate([jnp.zeros((N_GRP, 1), jnp.int32), cuts, live_rows[:, None]], axis=1)
        lens = bounds[:, 1:] - bounds[:, :-1]
        owners = jax.random.permutation(keys[4], N_GRP)
        starts = jnp.cumsum(counts) - counts
        slot_index = jnp.arange(slots_in, dtype=jnp.int32)
        flat_pos = starts[:, None] + slot_index[None, :]
        dest = jnp.where(slot_index[None, :] < counts[:, None], owners[flat_pos % N_GRP], -1)
        return (lens.astype(jnp.int32), dest.astype(jnp.int32))
    group_keys = jax.random.split(base, N_DP)
    lens, dest = jax.vmap(one_group)(group_keys)
    lens = jnp.transpose(lens, (1, 0, 2)).reshape(N_GRP * N_DP, DOCS)
    dest = jnp.transpose(dest, (1, 0, 2)).reshape(N_GRP * N_DP, slots_in)
    return (lens, dest)


def draw_lengths(key, part):
    return shared_layout(key)[0]


def draw_dest(key, part):
    return shared_layout(key)[1]


def draw_tokens(key, part):
    keys = jax.random.split(jax.random.fold_in(key, 31), 3)
    values = jnp.clip(jax.random.normal(keys[0], (TOKENS, D), jnp.float32), -4.0, 4.0)
    row_scale = jnp.exp(jax.random.uniform(keys[1], (TOKENS, 1), jnp.float32, 0.0, math.log(10.0)))
    col_scale = jnp.exp(jax.random.uniform(keys[2], (1, D), jnp.float32, math.log(0.3), math.log(3.0)))
    return (values * row_scale * col_scale).astype(jnp.bfloat16)


def block_scale(own_key, extent, shards, least, high):
    loudness = 1.0
    for dim, parts in shards:
        heights = jax.random.uniform(jax.random.fold_in(jax.random.fold_in(own_key, 6), dim), (parts,), jnp.float32, least / len(shards), high / len(shards))
        loudness = loudness * jnp.repeat(jnp.exp(heights), extent[dim] // parts).reshape((-1,) + (1,) * (len(extent) - 1 - dim))
    return loudness


def noise(own_key, extent, deviation, most, cuts=(), held_as=jnp.bfloat16):
    loudness = block_scale(own_key, extent, cuts, -0.22, 0.18) if cuts else 1.0
    values = jax.random.normal(own_key, extent, jnp.float32) * deviation * loudness
    return jnp.minimum(jnp.maximum(values, -most), most).astype(held_as)


def setup_inputs(seed: int = 0) -> dict:
    key_list = jax.random.split(jax.random.key(seed), 6)
    return {
        "tokens": draw_tokens(jax.random.fold_in(key_list[5], 71), 0),
        "lengths": draw_lengths(jax.random.fold_in(key_list[5], 71), 0),
        "dest": draw_dest(jax.random.fold_in(key_list[5], 71), 0),
        "gain": jnp.clip(1.0 + 0.1 * jax.random.normal(key_list[3], (D,), jnp.float32), 0.5, 1.5),
        "weight": noise(key_list[4], (D, FF), D ** -0.5, 0.09375, ((0, 32), (1, 16))),
    }


EPS = 1e-06

def normalize_source(rows, lens, gain):
    count = rows.shape[0]
    doc_ends = jnp.cumsum(lens)
    position = jnp.arange(count, dtype=jnp.int32)
    doc_index = lax.optimization_barrier(jnp.sum((position[:, None] >= doc_ends[None, :]).astype(jnp.int32), axis=1))
    is_live = position < doc_ends[-1]
    onehot = (doc_index[:, None] == jnp.arange(DOCS, dtype=jnp.int32)[None, :]) & is_live[:, None]
    widened = rows.astype(jnp.float32)
    square = lax.optimization_barrier(jnp.sum(widened * widened, axis=1))
    totals = lax.optimization_barrier(jnp.sum(jnp.where(onehot, square[:, None], jnp.float32(0.0)), axis=0))
    mean_square = totals / (jnp.maximum(lens, 1).astype(jnp.float32) * D)
    inverse = lax.rsqrt(mean_square + EPS)
    scale = lax.optimization_barrier(jnp.sum(jnp.where(onehot, inverse[None, :], jnp.float32(0.0)), axis=1))
    return (widened * scale[:, None] * gain[None, :]).astype(jnp.bfloat16)

def group_rows(tokens_grp, lens_grp, dest_grp, gain):
    normed = jax.vmap(normalize_source, in_axes=(0, 0, None))(tokens_grp, lens_grp, gain)
    blocks = normed.reshape(N_GRP * IN_BLK, BLK, D)
    flat_dest = dest_grp.reshape(-1)
    flat_index = jnp.arange(N_GRP * IN_BLK, dtype=jnp.int32)
    earlier = (flat_dest[:, None] == flat_dest[None, :]) & (flat_index[None, :] < flat_index[:, None])
    owner_rank = lax.optimization_barrier(jnp.sum(earlier.astype(jnp.int32), axis=1))
    matches = (flat_dest[:, None, None] == jnp.arange(N_GRP, dtype=jnp.int32)[None, :, None]) & (owner_rank[:, None, None] == jnp.arange(OWN_BLK, dtype=jnp.int32)[None, None, :])
    picked = lax.optimization_barrier(jnp.sum(jnp.where(matches, flat_index[:, None, None], 0), axis=0)).astype(jnp.int32)
    chosen = blocks[picked.reshape(-1)]
    return chosen.reshape(ROWS_GRP, D)

def reference(tokens, lengths, dest, gain, weight):
    token_groups = jnp.transpose(tokens.reshape(N_GRP, N_DP, IN_BLK * BLK, D), (1, 0, 2, 3))
    length_groups = jnp.transpose(lengths.reshape(N_GRP, N_DP, DOCS), (1, 0, 2))
    dest_groups = jnp.transpose(dest.reshape(N_GRP, N_DP, IN_BLK), (1, 0, 2))

    def per_group(items):
        rows = group_rows(items[0], items[1], items[2], gain)
        return jnp.dot(rows, weight, preferred_element_type=jnp.float32).astype(jnp.bfloat16)
    result = lax.map(per_group, (token_groups, length_groups, dest_groups))
    return result.reshape(N_DP * ROWS_GRP, FF)
```

```python
import jax
import jax.numpy as jnp
from jax import lax
from jax.experimental import pallas as pl
from jax.experimental.pallas import tpu as pltpu
from jax.sharding import PartitionSpec as P

BLK = 32
OWN_BLK = 2
EPS = 1e-06
LANES = 128


def norm_kernel(lens_ref, dest_ref, tokens_ref, gain_ref, *outs):
    rows, features = tokens_ref.shape
    slots = rows // BLK
    unit = 2
    pieces = BLK // unit
    per_piece = slots * unit
    x = tokens_ref[...].astype(jnp.float32)
    square = jnp.sum(x * x, axis=1, keepdims=True)
    row = lax.broadcasted_iota(jnp.int32, (rows, 1), 0)
    scale = jnp.zeros((rows, 1), jnp.float32)
    start = jnp.int32(0)
    for c in range(lens_ref.shape[1]):
        size = lens_ref[0, c]
        inside = (row >= start) & (row < start + size)
        total = jnp.sum(jnp.where(inside, square, 0.0), axis=0, keepdims=True)
        count = jnp.full((1, 1), jnp.maximum(size, 1) * features, jnp.int32).astype(jnp.float32)
        inverse = lax.rsqrt(total / count + EPS)
        scale = scale + jnp.where(inside, inverse, 0.0)
        start = start + size
    normed = (x * scale * gain_ref[...]).astype(jnp.bfloat16)
    to = lax.broadcasted_iota(jnp.int32, (rows, rows), 0)
    frm = lax.broadcasted_iota(jnp.int32, (rows, rows), 1)
    want = (to % per_piece) // unit * BLK + (to // per_piece) * unit + to % unit
    perm = (want == frm).astype(jnp.float32).astype(jnp.bfloat16)
    mixed = jnp.dot(perm, normed, preferred_element_type=jnp.float32).astype(jnp.bfloat16)
    at = 0
    for n, out in enumerate(outs):
        width = out.shape[1] - (LANES if n == 0 else 0)
        out[:, :width] = mixed[:, at : at + width]
        at += width
    slot = (lax.broadcasted_iota(jnp.int32, (rows, LANES), 0) % per_piece) // unit
    owner = jnp.full((rows, LANES), dest_ref[0, 0], jnp.int32)
    for k in range(1, slots):
        owner = jnp.where(slot == k, dest_ref[0, k], owner)
    outs[0][:, outs[0].shape[1] - LANES :] = owner.astype(jnp.float32).astype(jnp.bfloat16)


def place_kernel(groups, data_ref, out_ref):
    rows = data_ref.shape[0]
    picked, width = out_ref.shape
    owner = data_ref[:, width:].astype(jnp.float32)
    lane = lax.broadcasted_iota(jnp.int32, (rows, LANES), 1)
    same = ((owner == lane.astype(jnp.float32)) & (lane < groups)).astype(jnp.float32)
    to = lax.broadcasted_iota(jnp.int32, (rows, rows), 0)
    frm = lax.broadcasted_iota(jnp.int32, (rows, rows), 1)
    before = ((frm // 2 < to // 2) & (frm % 2 == 0)).astype(jnp.float32).astype(jnp.bfloat16)
    earlier = jnp.dot(before, same.astype(jnp.bfloat16), preferred_element_type=jnp.float32)
    rank = jnp.sum(earlier * same, axis=1, keepdims=True)
    live = jnp.sum(same, axis=1, keepdims=True) > 0.5
    half = (lax.broadcasted_iota(jnp.int32, (rows, 1), 0) % 2).astype(jnp.float32)
    target = (owner[:, :1] * OWN_BLK + rank) * 2.0 + half
    spot = lax.broadcasted_iota(jnp.int32, (rows, picked), 1).astype(jnp.float32)
    pick = ((spot == target) & live).astype(jnp.float32).astype(jnp.bfloat16)
    out_ref[...] = lax.dot_general(
        pick, data_ref[:, :width], (((0,), (0,)), ((), ())), preferred_element_type=jnp.float32
    ).astype(jnp.bfloat16)


CHUNKS = 4


def project_kernel(x_hbm, w_ref, out_hbm, x_buf, y_buf, in_sem, out_sem):
    pieces, picked, depth = x_hbm.shape
    part = picked // CHUNKS
    height = pieces * part

    def load(q):
        return pltpu.make_async_copy(
            x_hbm.at[:, pl.ds(q * part, part), :], x_buf.at[q % 2], in_sem.at[q % 2]
        )

    def store(q):
        return pltpu.make_async_copy(
            y_buf.at[q % 2], out_hbm.at[pl.ds(q * height, height), :], out_sem.at[q % 2]
        )

    to = lax.broadcasted_iota(jnp.int32, (height, height), 0)
    frm = lax.broadcasted_iota(jnp.int32, (height, height), 1)
    want = (to % BLK) // 2 * part + (to // BLK) * 2 + to % 2
    perm = (want == frm).astype(jnp.float32).astype(jnp.bfloat16)
    load(0).start()
    for q in range(CHUNKS):
        if q + 1 < CHUNKS:
            load(q + 1).start()
        load(q).wait()
        x = x_buf[q % 2].reshape(height, depth)
        y = jnp.dot(x, w_ref[...], preferred_element_type=jnp.float32).astype(jnp.bfloat16)
        if q >= 2:
            store(q - 2).wait()
        y_buf[q % 2] = jnp.dot(perm, y, preferred_element_type=jnp.float32).astype(jnp.bfloat16)
        store(q).start()
    for q in range(CHUNKS - 2, CHUNKS):
        store(q).wait()


def cost(flops, nbytes):
    return pl.CostEstimate(flops=flops, bytes_accessed=nbytes, transcendentals=0)


VM = pl.BlockSpec(memory_space=pltpu.VMEM)
SM = pl.BlockSpec(memory_space=pltpu.SMEM)
HB = pl.BlockSpec(memory_space=pltpu.HBM)
MIB = 1024 * 1024


def per_device(tokens, lengths, dest, gain, weight):
    groups = lax.axis_size("grp")
    rows, features = tokens.shape
    cols = weight.shape[1]
    own = groups * OWN_BLK * 2
    (mixed,) = pl.pallas_call(
        norm_kernel,
        out_shape=[jax.ShapeDtypeStruct((rows, features + LANES), jnp.bfloat16)],
        in_specs=[SM, SM, VM, VM],
        out_specs=[VM],
        compiler_params=pltpu.CompilerParams(vmem_limit_bytes=16 * MIB),
        cost_estimate=cost(2 * rows * rows * features, 4 * rows * features),
        name="norm",
    )(lengths, dest, tokens, gain.reshape(1, features))
    with jax.named_scope("swap"):
        sent = lax.all_to_all(mixed, "grp", split_axis=0, concat_axis=0, tiled=True)
    owned = pl.pallas_call(
        lambda *refs: place_kernel(groups, *refs),
        out_shape=jax.ShapeDtypeStruct((own, features), jnp.bfloat16),
        in_specs=[VM],
        out_specs=VM,
        compiler_params=pltpu.CompilerParams(vmem_limit_bytes=16 * MIB),
        cost_estimate=cost(2 * rows * own * features, 3 * rows * features),
        name="place",
    )(sent)
    with jax.named_scope("wide"):
        w_all = lax.all_gather(weight, "dp", axis=0, tiled=True)
    owned, w_all = lax.optimization_barrier((owned, w_all))
    with jax.named_scope("spread"):
        x_all = lax.all_gather(owned, "grp", axis=0, tiled=True)
    height = groups * own // CHUNKS
    return pl.pallas_call(
        project_kernel,
        out_shape=jax.ShapeDtypeStruct((groups * own, cols), jnp.bfloat16),
        in_specs=[HB, VM],
        out_specs=HB,
        scratch_shapes=[
            pltpu.VMEM((2, groups, own // CHUNKS, features), jnp.bfloat16),
            pltpu.VMEM((2, height, cols), jnp.bfloat16),
            pltpu.SemaphoreType.DMA((2,)),
            pltpu.SemaphoreType.DMA((2,)),
        ],
        compiler_params=pltpu.CompilerParams(vmem_limit_bytes=56 * MIB),
        cost_estimate=cost(2 * groups * own * features * cols, 2 * groups * own * features),
        name="project",
    )(x_all.reshape(groups, own, features), w_all)


def solution(mesh):
    placed = (
        P(("grp", "dp"), None),
        P(("grp", "dp"), None),
        P(("grp", "dp"), None),
        P(),
        P("dp", "grp"),
    )
    return jax.shard_map(
        per_device, mesh=mesh, in_specs=placed, out_specs=P("dp", "grp"), check_vma=False
    )
```

```python
import jax
import jax.numpy as jnp
from jax import lax
from jax.experimental import pallas as pl
from jax.experimental.pallas import tpu as pltpu
from jax.sharding import PartitionSpec as P

BLK = 32
OWN_BLK = 2
EPS = 1e-06
LANES = 128


def norm_kernel(
    lens_hbm, dest_hbm, tokens_hbm, gain_hbm, out_ref, lens_ref, dest_ref, tokens_ref, gain_ref, sems
):
    copies = [
        pltpu.make_async_copy(src, dst, sems.at[n])
        for n, (src, dst) in enumerate(
            (
                (tokens_hbm, tokens_ref),
                (gain_hbm, gain_ref.at[0]),
                (lens_hbm, lens_ref),
                (dest_hbm, dest_ref),
            )
        )
    ]
    for copy in copies:
        copy.start()
    rows, features = tokens_ref.shape
    slots = rows // BLK
    unit = 2
    per_piece = slots * unit
    to = lax.broadcasted_iota(jnp.int32, (rows, rows), 0)
    frm = lax.broadcasted_iota(jnp.int32, (rows, rows), 1)
    want = (to % per_piece) // unit * BLK + (to // per_piece) * unit + to % unit
    perm = (want == frm).astype(jnp.float32).astype(jnp.bfloat16)
    for copy in copies:
        copy.wait()
    x = tokens_ref[...].astype(jnp.float32)
    square = jnp.sum(x * x, axis=1, keepdims=True)
    row = lax.broadcasted_iota(jnp.int32, (rows, 1), 0)
    scale = jnp.zeros((rows, 1), jnp.float32)
    start = jnp.int32(0)
    for c in range(lens_ref.shape[1]):
        size = lens_ref[0, c]
        inside = (row >= start) & (row < start + size)
        total = jnp.sum(jnp.where(inside, square, 0.0), axis=0, keepdims=True)
        count = jnp.full((1, 1), jnp.maximum(size, 1) * features, jnp.int32).astype(jnp.float32)
        inverse = lax.rsqrt(total / count + EPS)
        scale = scale + jnp.where(inside, inverse, 0.0)
        start = start + size
    normed = (x * scale * gain_ref[...]).astype(jnp.bfloat16)
    out_ref[:, :features] = jnp.dot(
        perm, normed, preferred_element_type=jnp.float32
    ).astype(jnp.bfloat16)
    slot = (lax.broadcasted_iota(jnp.int32, (rows, LANES), 0) % per_piece) // unit
    owner = jnp.full((rows, LANES), dest_ref[0, 0], jnp.int32)
    for k in range(1, slots):
        owner = jnp.where(slot == k, dest_ref[0, k], owner)
    out_ref[:, features:] = owner.astype(jnp.float32).astype(jnp.bfloat16)


def place_kernel(groups, data_ref, out_ref):
    rows = data_ref.shape[0]
    picked, width = out_ref.shape
    owner = data_ref[:, width:].astype(jnp.float32)
    lane = lax.broadcasted_iota(jnp.int32, (rows, LANES), 1)
    same = ((owner == lane.astype(jnp.float32)) & (lane < groups)).astype(jnp.float32)
    to = lax.broadcasted_iota(jnp.int32, (rows, rows), 0)
    frm = lax.broadcasted_iota(jnp.int32, (rows, rows), 1)
    before = ((frm // 2 < to // 2) & (frm % 2 == 0)).astype(jnp.float32).astype(jnp.bfloat16)
    earlier = jnp.dot(before, same.astype(jnp.bfloat16), preferred_element_type=jnp.float32)
    rank = jnp.sum(earlier * same, axis=1, keepdims=True)
    live = jnp.sum(same, axis=1, keepdims=True) > 0.5
    half = (lax.broadcasted_iota(jnp.int32, (rows, 1), 0) % 2).astype(jnp.float32)
    target = (owner[:, :1] * OWN_BLK + rank) * 2.0 + half
    spot = lax.broadcasted_iota(jnp.int32, (rows, picked), 1).astype(jnp.float32)
    pick = ((spot == target) & live).astype(jnp.float32).astype(jnp.bfloat16)
    out_ref[...] = lax.dot_general(
        pick, data_ref[:, :width], (((0,), (0,)), ((), ())), preferred_element_type=jnp.float32
    ).astype(jnp.bfloat16)


HALVES = 2
PARTS = 2
STEP = 512


TILE = 256


def join_kernel(side_ref, mine_ref, theirs_ref, out_ref, whole, sems):
    side = side_ref[0]
    first = pltpu.make_async_copy(mine_ref, whole.at[:, side], sems.at[0])
    second = pltpu.make_async_copy(theirs_ref, whole.at[:, 1 - side], sems.at[1])
    first.start()
    second.start()
    first.wait()
    second.wait()
    cols, depth = out_ref.shape
    flat = whole.reshape(depth, cols)
    for k in range(0, depth, TILE):
        out_ref[:, k : k + TILE] = flat[k : k + TILE, :].T


def project_kernel(x_hbm, w_hbm, out_hbm, x_buf, w_buf, y_buf, x_sem, w_sem, out_sem):
    depth = x_hbm.shape[2]
    halves, parts, pieces, picked, _ = x_buf.shape
    height = pieces * picked

    def load(q, s, n):
        if q == 0:
            cut = pl.ds(n * STEP, STEP)
        else:
            cut = pl.ds(0, depth)
        rows = pl.ds((q * parts + s) * picked, picked)
        return pltpu.make_async_copy(
            x_hbm.at[:, rows, cut], x_buf.at[q, s, :, :, cut], x_sem.at[q, s, n]
        )

    def weights(n):
        cut = pl.ds(n * STEP, STEP)
        return pltpu.make_async_copy(w_hbm.at[:, cut], w_buf.at[:, cut], w_sem.at[n])

    steps = depth // STEP
    for n in range(steps):
        weights(n).start()
        for s in range(parts):
            load(0, s, n).start()
    for q in range(1, halves):
        for s in range(parts):
            load(q, s, 0).start()
    to = lax.broadcasted_iota(jnp.int32, (height, height), 0)
    frm = lax.broadcasted_iota(jnp.int32, (height, height), 1)
    want = (to % BLK) // 2 * picked + (to // BLK) * 2 + to % 2
    perm = (want == frm).astype(jnp.float32).astype(jnp.bfloat16)
    across = (((1,), (1,)), ((), ()))
    stores = []
    for q in range(halves):
        total = None
        width = STEP if q == 0 else depth
        for n in range(depth // width):
            if q == 0:
                weights(n).wait()
            for s in range(parts):
                load(q, s, n).wait()
            low, high = n * width, (n + 1) * width
            x = x_buf[q, :, :, :, low:high].reshape(parts * height, width)
            term = lax.dot_general(
                w_buf[:, low:high], x, across, preferred_element_type=jnp.float32
            )
            total = term if total is None else total + term
        y = total.astype(jnp.bfloat16)
        for s in range(parts):
            k = q * parts + s
            y_buf[k] = lax.dot_general(
                perm,
                y[:, s * height : (s + 1) * height],
                across,
                preferred_element_type=jnp.float32,
            ).astype(jnp.bfloat16)
            store = pltpu.make_async_copy(
                y_buf.at[k], out_hbm.at[pl.ds(k * height, height), :], out_sem.at[k]
            )
            store.start()
            stores.append(store)
    for store in stores:
        store.wait()


def cost(flops, nbytes):
    return pl.CostEstimate(flops=flops, bytes_accessed=nbytes, transcendentals=0)


VM = pl.BlockSpec(memory_space=pltpu.VMEM)
SM = pl.BlockSpec(memory_space=pltpu.SMEM)
HB = pl.BlockSpec(memory_space=pltpu.HBM)
MIB = 1024 * 1024


def per_device(tokens, lengths, dest, gain, weight):
    groups = lax.axis_size("grp")
    rows, features = tokens.shape
    cols = weight.shape[1]
    own = groups * OWN_BLK * 2
    mixed = pl.pallas_call(
        norm_kernel,
        out_shape=jax.ShapeDtypeStruct((rows, features + LANES), jnp.bfloat16),
        in_specs=[HB, HB, HB, HB],
        out_specs=VM,
        scratch_shapes=[
            pltpu.SMEM(lengths.shape, jnp.int32),
            pltpu.SMEM(dest.shape, jnp.int32),
            pltpu.VMEM(tokens.shape, jnp.bfloat16),
            pltpu.VMEM((1, features), jnp.float32),
            pltpu.SemaphoreType.DMA((4,)),
        ],
        compiler_params=pltpu.CompilerParams(vmem_limit_bytes=65800000),
        cost_estimate=cost(2 * rows * rows * features, 4 * rows * features),
        name="norm",
    )(lengths, dest, tokens, gain)
    with jax.named_scope("swap"):
        sent = lax.all_to_all(mixed, "grp", split_axis=0, concat_axis=0, tiled=True)
    owned = pl.pallas_call(
        lambda *refs: place_kernel(groups, *refs),
        out_shape=jax.ShapeDtypeStruct((own, features), jnp.bfloat16),
        in_specs=[VM],
        out_specs=VM,
        compiler_params=pltpu.CompilerParams(vmem_limit_bytes=16 * MIB),
        cost_estimate=cost(2 * rows * own * features, 3 * rows * features),
        name="place",
    )(sent)
    owned, weight = lax.optimization_barrier((owned, weight))
    with jax.named_scope("spread"):
        x_all = lax.all_gather(owned, "grp", axis=0, tiled=True)
    with jax.named_scope("wide"):
        depth = weight.shape[0]
        cores = lax.axis_size("dp") // 2
        copies = jnp.broadcast_to(weight[None], (cores, depth, cols)).reshape(cores * depth, cols)
        same = [[2 * i + c for i in range(cores)] for c in range(2)]
        mine = lax.all_to_all(
            copies, "dp", split_axis=0, concat_axis=0, tiled=True, axis_index_groups=same
        )
        theirs = lax.ppermute(mine, "dp", [(d, d ^ 1) for d in range(2 * cores)])
        w_all = pl.pallas_call(
            join_kernel,
            out_shape=jax.ShapeDtypeStruct((cols, features), jnp.bfloat16),
            in_specs=[SM, HB, HB],
            out_specs=VM,
            scratch_shapes=[
                pltpu.VMEM((cores, 2, depth, cols), jnp.bfloat16),
                pltpu.SemaphoreType.DMA((2,)),
            ],
            compiler_params=pltpu.CompilerParams(vmem_limit_bytes=24 * MIB),
            cost_estimate=cost(0, 4 * cores * depth * cols * 2),
            name="join",
        )(
            lax.rem(lax.axis_index("dp"), 2).reshape(1),
            mine.reshape(cores, depth, cols),
            theirs.reshape(cores, depth, cols),
        )
    count = HALVES * PARTS
    picked = own // count
    return pl.pallas_call(
        project_kernel,
        out_shape=jax.ShapeDtypeStruct((groups * own, cols), jnp.bfloat16),
        in_specs=[HB, HB],
        out_specs=HB,
        scratch_shapes=[
            pltpu.VMEM((HALVES, PARTS, groups, picked, features), jnp.bfloat16),
            pltpu.VMEM((cols, features), jnp.bfloat16),
            pltpu.VMEM((count, groups * picked, cols), jnp.bfloat16),
            pltpu.SemaphoreType.DMA((HALVES, PARTS, features // STEP)),
            pltpu.SemaphoreType.DMA((features // STEP,)),
            pltpu.SemaphoreType.DMA((count,)),
        ],
        compiler_params=pltpu.CompilerParams(vmem_limit_bytes=56 * MIB),
        cost_estimate=cost(2 * groups * own * features * cols, 2 * groups * own * features),
        name="project",
    )(x_all.reshape(groups, own, features), w_all)


def solution(mesh):
    placed = (
        P(("grp", "dp"), None),
        P(("grp", "dp"), None),
        P(("grp", "dp"), None),
        P(),
        P("dp", "grp"),
    )
    return jax.shard_map(
        per_device, mesh=mesh, in_specs=placed, out_specs=P("dp", "grp"), check_vma=False
    )
```
